32 devices in a mesh: expert: 4 (over x, core), shard: 8 (over z, y).
Axes of the slice: x: 2, y: 2, z: 4, core: 2. Of those that a mesh axis runs over, the one named last changes fastest.
Arguments:
- tokens: bfloat16 [48, 4096], P('shard', 'expert'), may hold values from -6 to 6
- expert_ids: int32 [48, 2], P('shard'), may hold values from 0 to 3, all different within a row; in each aligned block of 6 rows (0 to 5, 6 to 11, ...) at most 6 rows name the same one
- gates: float32 [48, 2], P('shard'), may hold values from 0.1 to 1
- gate_proj: bfloat16 [4, 4096, 8192], P('expert', None, 'shard'), may hold values from -0.09375 to 0.09375
- up_proj: bfloat16 [4, 4096, 8192], P('expert', None, 'shard'), may hold values from -0.09375 to 0.09375
- down_proj_t: bfloat16 [4, 4096, 8192], P('expert', 'shard'), may hold values from -0.0625 to 0.0625
Outputs:
- mixed: bfloat16 [48, 4096], P('shard', 'expert')
The draws below stay inside these ranges and needn't reach their ends.
Inputs may be any that keep to these rules, and one draw needn't show every extreme that they name: `expert_ids`: each token names two different experts; among the 6 tokens of one aligned block no expert is named more than 6 times, and in every draw some expert is named exactly 6 times in some block.
All inputs are finite; a program needn't handle non-finite values.
Results may differ from the reference program's by a relative error of at most 0.0085.
Values may be sent and summed in bfloat16 or wider, within the bound.
A program may use at most 64 MiB of HBM per device.

```python
import math
import jax
import jax.numpy as jnp
import numpy as np
from jax import lax

D = 4096
FF = 8192
TOK_SH = 6
EXPERTS = 4
CAP = 6
TOKENS = 48
N_SHARD = 8


def shard_levels(own_key, extent, pieces, least, top_value):
    gain = 1.0
    for dim, parts in pieces:
        heights = jax.random.uniform(jax.random.fold_in(jax.random.fold_in(own_key, 6), dim), (parts,), jnp.float32, least / len(pieces), top_value / len(pieces))
        gain = gain * jnp.repeat(jnp.exp(heights), extent[dim] // parts).reshape((-1,) + (1,) * (len(extent) - 1 - dim))
    return gain


def deal_out(rng, own, number, rows, count, top, bound, slope):
    sequence = jax.random.permutation(rng, count)
    crowded, usual = shares(count, rows * top, bound, slope, True), shares(count, rows * top, bound, slope, False)
    places = jnp.arange(count)

    def named(lengths, offset_by):
        used = int((lengths > 0).sum())
        fixed = max(1, used // 4)
        passed = fixed + (places - fixed + offset_by * (used - fixed)) % max(1, count - fixed)
        return jnp.zeros((count,), jnp.int32).at[sequence[jnp.where(places < fixed, places, passed)]].set(jnp.asarray(lengths, jnp.int32))

    lengths = jnp.where(number % 4 == 0, named(crowded, number // 4), named(usual, number - number // 4 - 1))
    mixed = jax.random.permutation(jax.random.fold_in(own, 3), count)
    source_of, taker = mixed[0:count // 2 * 2:2], mixed[1:count // 2 * 2:2]
    room = jnp.minimum(lengths[source_of] - 1, bound - lengths[taker]) // 2
    room = jnp.where((source_of == sequence[0]) | (taker == sequence[0]) | (lengths[taker] == 0), 0, jnp.maximum(room, 0))
    passed = jax.random.randint(jax.random.fold_in(own, 4), (count // 2,), 0, 1 << 20) % (room + 1)
    lengths = lengths.at[source_of].add(-passed).at[taker].add(passed)
    labels = jnp.searchsorted(jnp.cumsum(lengths), jnp.arange(rows * top), side="right").astype(jnp.int32)
    table = labels.reshape(top, rows).T
    table = table[jax.random.permutation(jax.random.fold_in(own, 1), rows)]
    offset_by = jax.random.randint(jax.random.fold_in(own, 2), (rows, 1), 0, top)
    return jnp.take_along_axis(table, (jnp.arange(top)[None, :] + offset_by) % top, axis=1)


def shares(number_of, total, most, skew, full):
    weights = [(1 << 20) // math.isqrt(standing ** skew) + 1 for standing in range(1, number_of + 1)]
    largest = most if full else min(most, max(-(-total // number_of), total * weights[0] // sum(weights)))
    least = 1 if total - largest >= number_of - 1 else 0
    given, surplus = [largest] + [least] * (number_of - 1), total - largest - least * (number_of - 1)
    while surplus > 0:
        free = [i for i in range(1, number_of) if given[i] < largest] or [i for i in range(1, number_of) if given[i] < most]
        pool, left = sum([weights[i] for i in free]), surplus
        for i in free:
            more = min(most - given[i], max(1, left * weights[i] // pool), surplus)
            given[i] = given[i] + more
            surplus = surplus - more
    return np.array(given)


def noise(key, extent, spread, reach, shards=(), held_as=jnp.bfloat16):
    array = jax.random.normal(key, extent, jnp.float32) * spread
    if len(shards) > 0:
        array = shard_levels(key, extent, shards, -0.22, 0.18) * array
    return jnp.clip(array, min=-reach, max=reach).astype(held_as)


def setup_inputs(seed: int = 0) -> dict:
    key_list = jax.random.split(jax.random.key(seed), 7)
    tokens = noise(key_list[0], (TOKENS, D), 1.0, 6.0, ((0, 8), (1, 4)))
    expert_ids_keys = jax.random.split(jax.random.fold_in(key_list[1], 1), TOKENS // TOK_SH)
    expert_ids_turns = jax.random.permutation(jax.random.fold_in(key_list[1], 3), TOKENS // TOK_SH)
    expert_ids = jax.vmap(lambda own, number: deal_out(jax.random.fold_in(key_list[1], 2), own, number, TOK_SH, EXPERTS, 2, CAP, 2))(expert_ids_keys, expert_ids_turns).reshape((TOKENS, 2))
    gates = jnp.clip(jnp.exp(math.log(1.0) - 2.3025851 * jax.random.uniform(key_list[2], (TOKENS, 2), jnp.float32) ** shard_levels(key_list[2], (TOKENS, 2), ((0, 8),), -0.2, 0.2)), 0.1, 1.0)
    gate_proj = noise(key_list[3], (EXPERTS, D, FF), D ** -0.5, 0.09375, ((0, 4), (2, 8)))
    up_proj = noise(key_list[4], (EXPERTS, D, FF), D ** -0.5, 0.09375, ((0, 4), (2, 8)))
    down_proj_t = noise(key_list[5], (EXPERTS, D, FF), FF ** -0.5, 0.0625, ((0, 4), (1, 8)))
    return dict(tokens=tokens, expert_ids=expert_ids, gates=gates, gate_proj=gate_proj, up_proj=up_proj, down_proj_t=down_proj_t)


def reference(tokens, expert_ids, gates, gate_proj, up_proj, down_proj_t):
    expert_range = jnp.arange(EXPERTS, dtype=jnp.int32)
    matches = expert_ids[:, :, None] == expert_range[None, None, :]
    routed = jnp.sum(matches.astype(jnp.int32), axis=1)
    weight = jnp.sum(gates[:, :, None] * matches.astype(jnp.float32), axis=1)
    blocked = routed.reshape(N_SHARD, TOK_SH, EXPERTS)
    slot_rank = (jnp.cumsum(blocked, axis=1) - blocked).reshape(TOKENS, EXPERTS)
    token_block = jnp.arange(TOKENS, dtype=jnp.int32) // TOK_SH
    target = token_block[:, None] * CAP + slot_rank
    row_ids = jnp.arange(N_SHARD * CAP, dtype=jnp.int32)
    mixed_sum = jnp.zeros((TOKENS, D), jnp.float32)
    for expert in range(EXPERTS):
        picker = ((target[:, expert][None, :] == row_ids[:, None]) & (routed[:, expert][None, :] > 0)).astype(jnp.float32)
        picked = jnp.dot(picker.astype(jnp.bfloat16), tokens, preferred_element_type=jnp.float32).astype(jnp.bfloat16)
        gate_out = jnp.dot(picked, gate_proj[expert], preferred_element_type=jnp.float32)
        up_out = jnp.dot(picked, up_proj[expert], preferred_element_type=jnp.float32)
        hidden = (jax.nn.silu(gate_out) * up_out).astype(jnp.bfloat16)
        expert_out = lax.dot_general(hidden, down_proj_t[expert], (((1,), (1,)), ((), ())), preferred_element_type=jnp.float32).astype(jnp.bfloat16)
        combiner = picker.T * weight[:, expert][:, None]
        mixed_sum = mixed_sum + jnp.dot(combiner, expert_out.astype(jnp.float32), precision=lax.Precision.HIGHEST)
    return mixed_sum.astype(jnp.bfloat16)
```

```python
import functools

import jax
import jax.numpy as jnp
from jax import lax
from jax.experimental import pallas as pl
from jax.experimental.pallas import tpu as pltpu
from jax.sharding import PartitionSpec as P

PAD = 8
MESH = pl.DeviceIdType.MESH
F32 = jnp.float32
BF16 = jnp.bfloat16


def flip(index, mask):
    bit, out = 1, index
    while bit <= mask:
        if mask & bit:
            out = out + bit - 2 * bit * ((index // bit) % 2)
        bit *= 2
    return out


def kernel(
    n_e, n_s, chunks,
    tok_ref, ids_ref, gates_ref, gate_hbm, up_hbm, down_hbm, out_ref,
    gbuf, ubuf, dbuf, x8, xc, gacc, uacc, hbuf, oacc, obuf, rbuf,
    wsem, dsem, a_send, a_recv, e_send, e_recv, h_send, h_fwd, h_recv, c_send, c_recv,
):
    e = lax.axis_index("expert")
    s = lax.axis_index("shard")
    tok, width = tok_ref.shape
    tokens = tok * n_s
    hid = gbuf.shape[2]
    wide = hid // chunks
    rows_out = dbuf.shape[1]
    group = n_s // n_e
    n_dev = n_e * n_s

    weight_copies, down_copies = [], []
    for r in range(n_e):
        rows = pl.ds(pl.multiple_of(flip(e, r) * width, width), width)
        pair = (
            pltpu.make_async_copy(gate_hbm.at[0, rows, :], gbuf.at[r], wsem.at[0, r]),
            pltpu.make_async_copy(up_hbm.at[0, rows, :], ubuf.at[r], wsem.at[1, r]),
        )
        for copy in pair:
            copy.start()
        weight_copies.append(pair)
    for q in range(n_s):
        columns = pl.ds(pl.multiple_of(flip(s, q) * hid, hid), hid)
        copy = pltpu.make_async_copy(down_hbm.at[0, :, columns], dbuf.at[q], dsem.at[q])
        copy.start()
        down_copies.append(copy)

    x8[s] = jnp.concatenate(
        [tok_ref[...].astype(F32), jnp.zeros((PAD - tok, width), F32)], axis=0
    ).astype(BF16)
    gacc[...] = jnp.zeros_like(gacc)
    uacc[...] = jnp.zeros_like(uacc)
    oacc[...] = jnp.zeros_like(oacc)

    barrier = pltpu.get_barrier_semaphore()
    me = e * n_s + s

    def greet(i, carry):
        other = lax.rem(me + i, n_dev)
        pl.semaphore_signal(
            barrier, inc=1, device_id=(other // n_s, other % n_s), device_id_type=MESH
        )
        return carry

    lax.fori_loop(1, n_dev, greet, 0)
    pl.semaphore_wait(barrier, n_dev - 1)

    sent = []

    def remote(src, dst, send, recv, device):
        return pltpu.make_async_remote_copy(
            src_ref=src, dst_ref=dst, send_sem=send, recv_sem=recv,
            device_id=device, device_id_type=MESH,
        )

    def push(*args):
        copy = remote(*args)
        copy.start()
        sent.append(copy)

    for q in sorted(range(1, n_s), reverse=True):
        push(x8.at[s], x8.at[s], a_send.at[q], a_recv.at[q], (e, flip(s, q)))
    for q in range(1, n_s):
        other = flip(s, q)
        remote(x8.at[other], x8.at[other], a_send.at[q], a_recv.at[q], (e, other)).wait_recv()

    padded = n_s * PAD
    i = lax.broadcasted_iota(jnp.int32, (tokens, padded), 0)
    j = lax.broadcasted_iota(jnp.int32, (tokens, padded), 1)
    block = lax.shift_right_logical(j, PAD.bit_length() - 1)
    pick = ((i == j - (PAD - tok) * block) & (j - PAD * block < tok)).astype(F32).astype(BF16)
    whole = x8[...].astype(F32).reshape(padded, width).astype(BF16)
    xc[0] = jnp.dot(pick, whole, preferred_element_type=F32).astype(BF16)

    partner = (flip(e, 1), s)
    for r in range(2, n_e, 2):
        push(xc.at[0], xc.at[r], e_send.at[r], e_recv.at[r], (flip(e, r), s))
    push(xc.at[0], xc.at[1], e_send.at[1], e_recv.at[1], partner)

    def arrived(r):
        remote(xc.at[r], xc.at[r], e_send.at[r], e_recv.at[r], partner).wait_recv()

    def project(r, last):
        for copy in weight_copies[r]:
            copy.wait()
        for c in range(chunks):
            columns = slice(c * wide, (c + 1) * wide)
            g = gacc[:, columns] + jnp.dot(xc[r], gbuf[r, :, columns], preferred_element_type=F32)
            u = uacc[:, columns] + jnp.dot(xc[r], ubuf[r, :, columns], preferred_element_type=F32)
            if not last:
                gacc[:, columns] = g
                uacc[:, columns] = u
                continue
            hbuf[0, c] = (g / (1.0 + jnp.exp(-g)) * u).astype(BF16)
            push(hbuf.at[0, c], hbuf.at[1, c], h_fwd.at[0, c], h_recv.at[1, c], (e, flip(s, 1)))
            for q in range(2, n_s, 2):
                push(hbuf.at[0, c], hbuf.at[q, c], h_send.at[q, c], h_recv.at[q, c], (e, flip(s, q)))

    project(0, n_e == 1)
    arrived(1)
    project(1, n_e == 2)
    for r in range(2, n_e, 2):
        arrived(r)
        push(xc.at[r], xc.at[r + 1], e_send.at[r + 1], e_recv.at[r + 1], partner)
        project(r, False)
    for r in range(3, n_e, 2):
        arrived(r)
        project(r, r == n_e - 1)

    waited = set()

    def down(q, c):
        if q not in waited:
            down_copies[q].wait()
            waited.add(q)
        oacc[...] += lax.dot_general(
            hbuf[q, c], dbuf[q, :, c * wide:(c + 1) * wide], (((1,), (1,)), ((), ())),
            preferred_element_type=F32,
        )

    def landed(q, c):
        remote(hbuf.at[q, c], hbuf.at[q, c], h_send.at[q, c], h_recv.at[q, c], partner).wait_recv()

    for c in range(chunks):
        down(0, c)
    for c in range(chunks):
        for q in range(2, n_s, 2):
            landed(q, c)
            push(hbuf.at[q, c], hbuf.at[q + 1, c], h_fwd.at[q, c], h_recv.at[q + 1, c], (e, flip(s, 1)))
            down(q, c)
        landed(1, c)
        down(1, c)
    for c in range(chunks):
        for q in range(3, n_s, 2):
            landed(q, c)
            down(q, c)

    spread = jnp.where((i == j - (PAD - tok) * block) & (j - PAD * block < tok), 1.0, 0.0).T.astype(BF16)
    blocks = jnp.dot(spread, oacc[...].astype(BF16), preferred_element_type=F32)
    obuf[...] = blocks.reshape(n_s, PAD, rows_out).astype(BF16)
    owner = s // group
    slot = e * group + lax.rem(s, group)
    own = e == owner

    @pl.when(own)
    def _():
        keep = pltpu.make_async_copy(obuf.at[s], rbuf.at[slot], c_recv.at[slot])
        keep.start()

    @pl.when(jnp.logical_not(own))
    def _():
        remote(obuf.at[s], rbuf.at[slot], c_send.at[0], c_recv.at[slot], (owner, s)).start()

    for q in range(1, n_s):
        other = flip(s, q)
        push(obuf.at[other], rbuf.at[slot], c_send.at[q], c_recv.at[slot], (owner, other))

    ids = ids_ref[...]
    gates = gates_ref[...]
    for copy in sent[:len(sent) - (n_s - 1)]:
        copy.wait_send()
    totals = [jnp.zeros((tok, rows_out), F32) for _ in range(group)]
    for x in range(n_e):
        weight = jnp.sum(jnp.where(ids == x, gates, 0.0), axis=1, keepdims=True)
        for k in range(group):
            n = x * group + k
            remote(rbuf.at[n], rbuf.at[n], c_send.at[0], c_recv.at[n], partner).wait_recv()
            totals[k] = totals[k] + weight * rbuf[n].astype(F32)[:tok]
    for k in range(group):
        out_ref[:, k * rows_out:(k + 1) * rows_out] = totals[k].astype(BF16)

    @pl.when(jnp.logical_not(own))
    def _():
        remote(obuf.at[s], rbuf.at[slot], c_send.at[0], c_recv.at[slot], (owner, s)).wait_send()

    for copy in sent[len(sent) - (n_s - 1):]:
        copy.wait_send()


def shards(n_e, n_s, tokens, expert_ids, gates, gate_proj, up_proj, down_proj_t):
    tok, width = tokens.shape
    _, _, hid = gate_proj.shape
    _, rows_out, _ = down_proj_t.shape
    chunks = max(1, hid // 256)
    wide = hid // chunks
    total = tok * n_s
    group = n_s // n_e
    dma = pltpu.SemaphoreType.DMA
    vmem = pl.BlockSpec(memory_space=pltpu.VMEM)
    hbm = pl.BlockSpec(memory_space=pl.ANY)
    return pl.pallas_call(
        functools.partial(kernel, n_e, n_s, chunks),
        out_shape=jax.ShapeDtypeStruct((tok, width), BF16),
        in_specs=[vmem, vmem, vmem, hbm, hbm, hbm],
        out_specs=vmem,
        scratch_shapes=[
            pltpu.VMEM((n_e, width, hid), BF16),
            pltpu.VMEM((n_e, width, hid), BF16),
            pltpu.VMEM((n_s, rows_out, hid), BF16),
            pltpu.VMEM((n_s, PAD, width), BF16),
            pltpu.VMEM((n_e, total, width), BF16),
            pltpu.VMEM((total, hid), F32),
            pltpu.VMEM((total, hid), F32),
            pltpu.VMEM((n_s, chunks, total, wide), BF16),
            pltpu.VMEM((total, rows_out), F32),
            pltpu.VMEM((n_s, PAD, rows_out), BF16),
            pltpu.VMEM((n_e * group, PAD, rows_out), BF16),
            dma((2, n_e)),
            dma((n_s,)),
            dma((n_s,)),
            dma((n_s,)),
            dma((n_e,)),
            dma((n_e,)),
            dma((n_s, chunks)),
            dma((n_s, chunks)),
            dma((n_s, chunks)),
            dma((n_s,)),
            dma((n_e * group,)),
        ],
        compiler_params=pltpu.CompilerParams(
            collective_id=0, has_side_effects=True, vmem_limit_bytes=60 * 1024 * 1024
        ),
    )(tokens, expert_ids, gates, gate_proj, up_proj, down_proj_t)


def solution(mesh):
    in_specs = (
        P("shard", "expert"),
        P("shard", None),
        P("shard", None),
        P("expert", None, "shard"),
        P("expert", None, "shard"),
        P("expert", "shard", None),
    )
    out_specs = P("shard", "expert")
    body = functools.partial(shards, mesh.shape["expert"], mesh.shape["shard"])
    return jax.shard_map(body, mesh=mesh, in_specs=in_specs, out_specs=out_specs, check_vma=False)
```

```python
import functools

import jax
import jax.numpy as jnp
from jax import lax
from jax.experimental import pallas as pl
from jax.experimental.pallas import tpu as pltpu
from jax.sharding import PartitionSpec as P

PAD = 8
MESH = pl.DeviceIdType.MESH
F32 = jnp.float32
BF16 = jnp.bfloat16


def flip(index, mask):
    bit, out = 1, index
    while bit <= mask:
        if mask & bit:
            out = out + bit - 2 * bit * ((index // bit) % 2)
        bit *= 2
    return out


def kernel(
    n_e, n_s, chunks,
    tok_ref, ids_ref, gates_ref, gate_hbm, up_hbm, down_hbm, out_ref,
    gbuf, ubuf, dbuf, x8, gacc, uacc, hbuf, oacc, obuf, rbuf,
    wsem, dsem, a_send, a_recv, h_send, h_fwd, h_recv, c_send, c_recv,
):
    e = lax.axis_index("expert")
    s = lax.axis_index("shard")
    tok, width = tok_ref.shape
    tokens = tok * n_s
    hid = gbuf.shape[2]
    wide = hid // chunks
    rows_out = dbuf.shape[1]
    group = n_s // n_e
    n_dev = n_e * n_s

    weight_copies, down_copies = [], []
    for r in range(n_e):
        rows = pl.ds(pl.multiple_of(flip(e, r) * width, width), width)
        pair = (
            pltpu.make_async_copy(gate_hbm.at[0, rows, :], gbuf.at[r], wsem.at[0, r]),
            pltpu.make_async_copy(up_hbm.at[0, rows, :], ubuf.at[r], wsem.at[1, r]),
        )
        for copy in pair:
            copy.start()
        weight_copies.append(pair)
    for q in range(n_s):
        columns = slice(q * hid, (q + 1) * hid)
        copy = pltpu.make_async_copy(down_hbm.at[0, :, columns], dbuf.at[q], dsem.at[q])
        copy.start()
        down_copies.append(copy)

    x8[0, s] = jnp.concatenate(
        [tok_ref[...].astype(F32), jnp.zeros((PAD - tok, width), F32)], axis=0
    ).astype(BF16)
    gacc[...] = jnp.zeros_like(gacc)
    uacc[...] = jnp.zeros_like(uacc)
    oacc[...] = jnp.zeros_like(oacc)

    barrier = pltpu.get_barrier_semaphore()
    me = e * n_s + s

    def greet(i, carry):
        other = lax.rem(me + i, n_dev)
        pl.semaphore_signal(
            barrier, inc=1, device_id=(other // n_s, other % n_s), device_id_type=MESH
        )
        return carry

    lax.fori_loop(1, n_dev, greet, 0)
    pl.semaphore_wait(barrier, n_dev - 1)

    sent = []

    def remote(src, dst, send, recv, device):
        return pltpu.make_async_remote_copy(
            src_ref=src, dst_ref=dst, send_sem=send, recv_sem=recv,
            device_id=device, device_id_type=MESH,
        )

    def push(*args):
        copy = remote(*args)
        copy.start()
        sent.append(copy)

    partner = (flip(e, 1), s)

    def onward(block):
        for r in range(2, n_e, 2):
            push(x8.at[0, block], x8.at[r, block], a_send.at[r, block], a_recv.at[r, block], (flip(e, r), s))
        push(x8.at[0, block], x8.at[1, block], a_send.at[1, block], a_recv.at[1, block], partner)

    def arrived(r, block):
        view = x8.at[r, block]
        remote(view, view, a_send.at[r, block], a_recv.at[r, block], partner).wait_recv()

    for q in sorted(range(1, n_s), reverse=True):
        push(x8.at[0, s], x8.at[0, s], a_send.at[0, flip(s, q)], a_recv.at[0, s], (e, flip(s, q)))
    onward(s)
    for q in range(1, n_s):
        block = flip(s, q)
        arrived(0, block)
        onward(block)

    padded = n_s * PAD
    i = lax.broadcasted_iota(jnp.int32, (tokens, padded), 0)
    j = lax.broadcasted_iota(jnp.int32, (tokens, padded), 1)
    block_of = lax.shift_right_logical(j, PAD.bit_length() - 1)
    pick = ((i == j - (PAD - tok) * block_of) & (j - PAD * block_of < tok)).astype(F32).astype(BF16)
    line, side = s // 2, lax.rem(s, 2)
    across = (e, flip(s, 1))
    n_line = n_s // 2

    def send_along(place, c, step, k):
        beside = line + step

        @pl.when((beside >= 0) & (beside < n_line))
        def _():
            remote(hbuf.at[place, c], hbuf.at[place, c], h_send.at[k, place, c], h_recv.at[place, c],
                   (e, s + 2 * step)).start()

    def send_across(place, c):
        remote(hbuf.at[place, c], hbuf.at[place, c], h_fwd.at[place, c], h_recv.at[place, c], across).start()

    def project(r, last):
        whole = x8[r].astype(F32).reshape(padded, width).astype(BF16)
        rows = jnp.dot(pick, whole, preferred_element_type=F32).astype(BF16)
        for copy in weight_copies[r]:
            copy.wait()
        for c in range(chunks):
            columns = slice(c * wide, (c + 1) * wide)
            g = gacc[:, columns] + jnp.dot(rows, gbuf[r, :, columns], preferred_element_type=F32)
            u = uacc[:, columns] + jnp.dot(rows, ubuf[r, :, columns], preferred_element_type=F32)
            if not last:
                gacc[:, columns] = g
                uacc[:, columns] = u
                continue
            hbuf[s, c] = (g / (1.0 + jnp.exp(-g)) * u).astype(BF16)
            send_across(s, c)
            send_along(s, c, 1, 0)
            send_along(s, c, -1, 1)

    project(0, n_e == 1)
    for q in range(n_s):
        arrived(1, flip(s, q))
    project(1, n_e == 2)
    for r in range(2, n_e, 2):
        for q in range(n_s):
            block = flip(s, q)
            arrived(r, block)
            push(x8.at[r, block], x8.at[r + 1, block], a_send.at[r + 1, block], a_recv.at[r + 1, block], partner)
        project(r, False)
    for r in range(3, n_e, 2):
        for q in range(n_s):
            arrived(r, flip(s, q))
        project(r, r == n_e - 1)

    for copy in down_copies:
        copy.wait()

    def down(place, c):
        columns = pl.ds(pl.multiple_of(c * wide, wide), wide)
        oacc[...] += lax.dot_general(
            hbuf[place, c], dbuf[place, :, columns], (((1,), (1,)), ((), ())),
            preferred_element_type=F32,
        )

    def landed(place, c):
        view = hbuf.at[place, c]
        remote(view, view, h_fwd.at[place, c], h_recv.at[place, c], across).wait_recv()

    inner = jnp.minimum(line, n_line - 1 - line)
    roomy = 1 - 2 * (line // ((n_line + 1) // 2))

    def event(t):
        paired = t < 2 * inner * chunks
        late = t - 2 * inner * chunks
        pair = t // 2
        away = jnp.where(paired, pair // chunks + 1, inner + 1 + late // chunks)
        c = jnp.where(paired, lax.rem(pair, chunks), lax.rem(late, chunks))
        sign = jnp.where(paired, 1 - 2 * lax.rem(t, 2), roomy)
        return line + sign * away, c, sign

    for c in range(chunks):
        down(s, c)

    steps = (n_line - 1) * chunks
    first = min(chunks, steps)

    def along(t):
        spot, c, sign = event(t)
        place = 2 * spot + side
        landed(place, c)
        send_along(place, c, -sign, 0)
        send_across(place, c)
        down(place, c)

    def beside_own(c):
        landed(flip(s, 1), c)
        down(flip(s, 1), c)

    def beside(t):
        spot, c, _ = event(t)
        place = 2 * spot + 1 - side
        landed(place, c)
        down(place, c)

    @pl.loop(0, first)
    def _(t):
        along(t)
        beside_own(t)

    @pl.loop(first, steps)
    def _(t):
        along(t)
        beside(t - first)

    @pl.loop(steps - first, steps)
    def _(t):
        beside(t)

    spread = pick.astype(F32).T.astype(BF16)
    blocks = jnp.dot(spread, oacc[...].astype(BF16), preferred_element_type=F32)
    obuf[...] = blocks.reshape(n_s, PAD, rows_out).astype(BF16)
    owner = s // group
    slot = e * group + lax.rem(s, group)
    own = e == owner

    @pl.when(own)
    def _():
        keep = pltpu.make_async_copy(obuf.at[s], rbuf.at[slot], c_recv.at[slot])
        keep.start()

    @pl.when(jnp.logical_not(own))
    def _():
        remote(obuf.at[s], rbuf.at[slot], c_send.at[0], c_recv.at[slot], (owner, s)).start()

    for q in range(1, n_s):
        other = flip(s, q)
        push(obuf.at[other], rbuf.at[slot], c_send.at[q], c_recv.at[slot], (owner, other))

    ids = ids_ref[...]
    gates = gates_ref[...]
    diagonal = lax.broadcasted_iota(jnp.int32, (tok, tok), 0) == lax.broadcasted_iota(jnp.int32, (tok, tok), 1)
    for copy in sent[:len(sent) - (n_s - 1)]:
        copy.wait_send()

    @pl.loop(0, chunks)
    def _(c):
        for k, step in ((0, 1), (1, -1)):
            beside_me = line + step

            @pl.when((beside_me >= 0) & (beside_me < n_line))
            def _():
                remote(hbuf.at[s, c], hbuf.at[s, c], h_send.at[k, s, c], h_recv.at[s, c], across).wait_send()

        remote(hbuf.at[s, c], hbuf.at[s, c], h_fwd.at[s, c], h_recv.at[s, c], across).wait_send()

    @pl.loop(0, steps)
    def _(t):
        spot, c, sign = event(t)
        place = 2 * spot + side
        view = hbuf.at[place, c]
        beside_me = line - sign

        @pl.when((beside_me >= 0) & (beside_me < n_line))
        def _():
            remote(view, view, h_send.at[0, place, c], h_recv.at[place, c], across).wait_send()

        remote(view, view, h_fwd.at[place, c], h_recv.at[place, c], across).wait_send()

    totals = [jnp.zeros((tok, rows_out), F32) for _ in range(group)]
    for x in range(n_e):
        row = jnp.sum(jnp.where(ids == x, gates, 0.0), axis=0, keepdims=True)
        weight = jnp.sum(jnp.where(diagonal, row, 0.0), axis=1, keepdims=True)
        for k in range(group):
            n = x * group + k
            remote(rbuf.at[n], rbuf.at[n], c_send.at[0], c_recv.at[n], partner).wait_recv()
            totals[k] = totals[k] + weight * rbuf[n].astype(F32)[:tok]
    for k in range(group):
        out_ref[:, k * rows_out:(k + 1) * rows_out] = totals[k].astype(BF16)

    @pl.when(jnp.logical_not(own))
    def _():
        remote(obuf.at[s], rbuf.at[slot], c_send.at[0], c_recv.at[slot], (owner, s)).wait_send()

    for copy in sent[len(sent) - (n_s - 1):]:
        copy.wait_send()


def shards(n_e, n_s, tokens, expert_ids, gates, gate_proj, up_proj, down_proj_t):
    tok, width = tokens.shape
    _, _, hid = gate_proj.shape
    _, rows_out, _ = down_proj_t.shape
    chunks = max(1, hid // 256)
    wide = hid // chunks
    total = tok * n_s
    group = n_s // n_e
    dma = pltpu.SemaphoreType.DMA
    vmem = pl.BlockSpec(memory_space=pltpu.VMEM)
    hbm = pl.BlockSpec(memory_space=pl.ANY)
    return pl.pallas_call(
        functools.partial(kernel, n_e, n_s, chunks),
        out_shape=jax.ShapeDtypeStruct((tok, width), BF16),
        in_specs=[vmem, vmem, vmem, hbm, hbm, hbm],
        out_specs=vmem,
        scratch_shapes=[
            pltpu.VMEM((n_e, width, hid), BF16),
            pltpu.VMEM((n_e, width, hid), BF16),
            pltpu.VMEM((n_s, rows_out, hid), BF16),
            pltpu.VMEM((n_e, n_s, PAD, width), BF16),
            pltpu.VMEM((total, hid), F32),
            pltpu.VMEM((total, hid), F32),
            pltpu.VMEM((n_s, chunks, total, wide), BF16),
            pltpu.VMEM((total, rows_out), F32),
            pltpu.VMEM((n_s, PAD, rows_out), BF16),
            pltpu.VMEM((n_e * group, PAD, rows_out), BF16),
            dma((2, n_e)),
            dma((n_s,)),
            dma((n_e, n_s)),
            dma((n_e, n_s)),
            dma((2, n_s, chunks)),
            dma((n_s, chunks)),
            dma((n_s, chunks)),
            dma((n_s,)),
            dma((n_e * group,)),
        ],
        compiler_params=pltpu.CompilerParams(
            collective_id=0, has_side_effects=True, vmem_limit_bytes=60 * 1024 * 1024
        ),
    )(tokens, expert_ids.T, gates.T, gate_proj, up_proj, down_proj_t)


def solution(mesh):
    in_specs = (
        P("shard", "expert"),
        P("shard", None),
        P("shard", None),
        P("expert", None, "shard"),
        P("expert", None, "shard"),
        P("expert", "shard", None),
    )
    out_specs = P("shard", "expert")
    body = functools.partial(shards, mesh.shape["expert"], mesh.shape["shard"])
    return jax.shard_map(body, mesh=mesh, in_specs=in_specs, out_specs=out_specs, check_vma=False)
```

```python
import functools

import jax
import jax.numpy as jnp
from jax import lax
from jax.experimental import pallas as pl
from jax.experimental.pallas import tpu as pltpu
from jax.sharding import PartitionSpec as P

PAD = 8
MESH = pl.DeviceIdType.MESH
F32 = jnp.float32
BF16 = jnp.bfloat16


def flip(index, mask):
    bit, out = 1, index
    while bit <= mask:
        if mask & bit:
            out = out + bit - 2 * bit * ((index // bit) % 2)
        bit *= 2
    return out


def kernel(
    n_e, n_s, chunks,
    tok_ref, ids_ref, gates_ref, gate_hbm, up_hbm, down_hbm, out_ref,
    gbuf, ubuf, dbuf, x8, gacc, uacc, hbuf, oacc, obuf, rbuf,
    wsem, dsem, a_send, a_recv, h_send, h_fwd, h_recv, c_send, c_recv,
):
    e = lax.axis_index("expert")
    s = lax.axis_index("shard")
    tok, width = tok_ref.shape
    tokens = tok * n_s
    hid = gbuf.shape[2]
    wide = hid // chunks
    rows_out = dbuf.shape[1]
    group = n_s // n_e
    n_dev = n_e * n_s

    weight_copies, down_copies = [], []
    for r in range(n_e):
        rows = pl.ds(pl.multiple_of(flip(e, r) * width, width), width)
        pair = (
            pltpu.make_async_copy(gate_hbm.at[0, rows, :], gbuf.at[r], wsem.at[0, r]),
            pltpu.make_async_copy(up_hbm.at[0, rows, :], ubuf.at[r], wsem.at[1, r]),
        )
        for copy in pair:
            copy.start()
        weight_copies.append(pair)
    for q in range(n_s):
        columns = slice(q * hid, (q + 1) * hid)
        copy = pltpu.make_async_copy(down_hbm.at[0, :, columns], dbuf.at[q], dsem.at[q])
        copy.start()
        down_copies.append(copy)

    x8[0, s] = jnp.concatenate(
        [tok_ref[...].astype(F32), jnp.zeros((PAD - tok, width), F32)], axis=0
    ).astype(BF16)
    gacc[...] = jnp.zeros_like(gacc)
    uacc[...] = jnp.zeros_like(uacc)
    oacc[...] = jnp.zeros_like(oacc)

    barrier = pltpu.get_barrier_semaphore()
    me = e * n_s + s

    def greet(i, carry):
        other = lax.rem(me + i, n_dev)
        pl.semaphore_signal(
            barrier, inc=1, device_id=(other // n_s, other % n_s), device_id_type=MESH
        )
        return carry

    lax.fori_loop(1, n_dev, greet, 0)
    pl.semaphore_wait(barrier, n_dev - 1)

    sent = []

    def remote(src, dst, send, recv, device):
        return pltpu.make_async_remote_copy(
            src_ref=src, dst_ref=dst, send_sem=send, recv_sem=recv,
            device_id=device, device_id_type=MESH,
        )

    def push(*args):
        copy = remote(*args)
        copy.start()
        sent.append(copy)

    partner = (flip(e, 1), s)

    def onward(block):
        for r in range(2, n_e, 2):
            push(x8.at[0, block], x8.at[r, block], a_send.at[r, block], a_recv.at[r, block], (flip(e, r), s))
        push(x8.at[0, block], x8.at[1, block], a_send.at[1, block], a_recv.at[1, block], partner)

    def arrived(r, block):
        view = x8.at[r, block]
        remote(view, view, a_send.at[r, block], a_recv.at[r, block], partner).wait_recv()

    for q in sorted(range(1, n_s), reverse=True):
        push(x8.at[0, s], x8.at[0, s], a_send.at[0, flip(s, q)], a_recv.at[0, s], (e, flip(s, q)))
    onward(s)
    for q in range(1, n_s):
        block = flip(s, q)
        arrived(0, block)
        onward(block)

    padded = n_s * PAD
    i = lax.broadcasted_iota(jnp.int32, (tokens, padded), 0)
    j = lax.broadcasted_iota(jnp.int32, (tokens, padded), 1)
    block_of = lax.shift_right_logical(j, PAD.bit_length() - 1)
    pick = ((i == j - (PAD - tok) * block_of) & (j - PAD * block_of < tok)).astype(F32).astype(BF16)
    line, side = s // 2, lax.rem(s, 2)
    across = (e, flip(s, 1))
    n_line = n_s // 2

    def send_along(place, c, step, k):
        beside = line + step

        @pl.when((beside >= 0) & (beside < n_line))
        def _():
            remote(hbuf.at[place, c], hbuf.at[place, c], h_send.at[k, place, c], h_recv.at[place, c],
                   (e, s + 2 * step)).start()

    def send_across(place, c):
        remote(hbuf.at[place, c], hbuf.at[place, c], h_fwd.at[place, c], h_recv.at[place, c], across).start()

    def project(r, last):
        whole = x8[r].astype(F32).reshape(padded, width).astype(BF16)
        rows = jnp.dot(pick, whole, preferred_element_type=F32).astype(BF16)
        for copy in weight_copies[r]:
            copy.wait()
        for c in range(chunks):
            columns = slice(c * wide, (c + 1) * wide)
            g = gacc[:, columns] + jnp.dot(rows, gbuf[r, :, columns], preferred_element_type=F32)
            u = uacc[:, columns] + jnp.dot(rows, ubuf[r, :, columns], preferred_element_type=F32)
            if not last:
                gacc[:, columns] = g
                uacc[:, columns] = u
                continue
            hbuf[s, c] = (g / (1.0 + jnp.exp(-g)) * u).astype(BF16)
            send_across(s, c)
            send_along(s, c, 1, 0)
            send_along(s, c, -1, 1)

    project(0, n_e == 1)
    for q in range(n_s):
        arrived(1, flip(s, q))
    project(1, n_e == 2)
    for r in range(2, n_e, 2):
        for q in range(n_s):
            block = flip(s, q)
            arrived(r, block)
            push(x8.at[r, block], x8.at[r + 1, block], a_send.at[r + 1, block], a_recv.at[r + 1, block], partner)
        project(r, False)
    for r in range(3, n_e, 2):
        for q in range(n_s):
            arrived(r, flip(s, q))
        project(r, r == n_e - 1)

    for copy in down_copies:
        copy.wait()

    def down(place, c):
        columns = pl.ds(pl.multiple_of(c * wide, wide), wide)
        oacc[...] += lax.dot_general(
            hbuf[place, c], dbuf[place, :, columns], (((1,), (1,)), ((), ())),
            preferred_element_type=F32,
        )

    def landed(place, c):
        view = hbuf.at[place, c]
        remote(view, view, h_fwd.at[place, c], h_recv.at[place, c], across).wait_recv()

    inner = jnp.minimum(line, n_line - 1 - line)
    roomy = 1 - 2 * (line // ((n_line + 1) // 2))

    def event(t):
        paired = t < 2 * inner * chunks
        late = t - 2 * inner * chunks
        pair = t // 2
        away = jnp.where(paired, pair // chunks + 1, inner + 1 + late // chunks)
        c = jnp.where(paired, lax.rem(pair, chunks), lax.rem(late, chunks))
        sign = jnp.where(paired, 1 - 2 * lax.rem(t, 2), roomy)
        return line + sign * away, c, sign

    steps = (n_line - 1) * chunks

    def across_piece(t):
        spot, c, _ = event(t)
        return 2 * spot + 1 - side, c

    def along_piece(t):
        spot, c, _ = event(t)
        return 2 * spot + side, c

    def together(pieces, wait):
        total = oacc[...]
        for place, c in pieces:
            if wait:
                landed(place, c)
            columns = pl.ds(pl.multiple_of(c * wide, wide), wide)
            total += lax.dot_general(
                hbuf[place, c], dbuf[place, :, columns], (((1,), (1,)), ((), ())),
                preferred_element_type=F32,
            )
        oacc[...] = total

    def relay(t):
        spot, c, sign = event(t)
        place = 2 * spot + side
        landed(place, c)
        send_along(place, c, -sign, 0)
        send_across(place, c)

    first = min(chunks, steps)

    @pl.loop(0, first)
    def _(t):
        relay(t)
        down(s, t)

    for c in range(first, chunks):
        down(s, c)

    second = min(2 * chunks, steps)

    @pl.loop(first, second)
    def _(t):
        relay(t)
        landed(flip(s, 1), t - first)
        down(flip(s, 1), t - first)

    for c in range(second - first, chunks):
        landed(flip(s, 1), c)
        down(flip(s, 1), c)

    @pl.loop(second, steps)
    def _(t):
        relay(t)
        down(*along_piece(t - second))

    done = (steps - second) // chunks

    @pl.loop(done, n_line - 1)
    def _(k):
        together([along_piece(k * chunks + c) for c in range(chunks)], False)

    @pl.loop(0, n_line - 1)
    def _(k):
        together([across_piece(k * chunks + c) for c in range(chunks)], True)

    spread = pick.astype(F32).T.astype(BF16)
    blocks = jnp.dot(spread, oacc[...].astype(BF16), preferred_element_type=F32)
    obuf[...] = blocks.reshape(n_s, PAD, rows_out).astype(BF16)
    owner = s // group
    slot = e * group + lax.rem(s, group)
    own = e == owner

    @pl.when(own)
    def _():
        keep = pltpu.make_async_copy(obuf.at[s], rbuf.at[slot], c_recv.at[slot])
        keep.start()

    @pl.when(jnp.logical_not(own))
    def _():
        remote(obuf.at[s], rbuf.at[slot], c_send.at[0], c_recv.at[slot], (owner, s)).start()

    for q in range(1, n_s):
        other = flip(s, q)
        push(obuf.at[other], rbuf.at[slot], c_send.at[q], c_recv.at[slot], (owner, other))

    ids = ids_ref[...]
    gates = gates_ref[...]
    diagonal = lax.broadcasted_iota(jnp.int32, (tok, tok), 0) == lax.broadcasted_iota(jnp.int32, (tok, tok), 1)
    for copy in sent[:len(sent) - (n_s - 1)]:
        copy.wait_send()

    @pl.loop(0, chunks)
    def _(c):
        for k, step in ((0, 1), (1, -1)):
            beside_me = line + step

            @pl.when((beside_me >= 0) & (beside_me < n_line))
            def _():
                remote(hbuf.at[s, c], hbuf.at[s, c], h_send.at[k, s, c], h_recv.at[s, c], across).wait_send()

        remote(hbuf.at[s, c], hbuf.at[s, c], h_fwd.at[s, c], h_recv.at[s, c], across).wait_send()

    @pl.loop(0, steps)
    def _(t):
        spot, c, sign = event(t)
        place = 2 * spot + side
        view = hbuf.at[place, c]
        beside_me = line - sign

        @pl.when((beside_me >= 0) & (beside_me < n_line))
        def _():
            remote(view, view, h_send.at[0, place, c], h_recv.at[place, c], across).wait_send()

        remote(view, view, h_fwd.at[place, c], h_recv.at[place, c], across).wait_send()

    totals = [jnp.zeros((tok, rows_out), F32) for _ in range(group)]
    for x in range(n_e):
        row = jnp.sum(jnp.where(ids == x, gates, 0.0), axis=0, keepdims=True)
        weight = jnp.sum(jnp.where(diagonal, row, 0.0), axis=1, keepdims=True)
        for k in range(group):
            n = x * group + k
            remote(rbuf.at[n], rbuf.at[n], c_send.at[0], c_recv.at[n], partner).wait_recv()
            totals[k] = totals[k] + weight * rbuf[n].astype(F32)[:tok]
    for k in range(group):
        out_ref[:, k * rows_out:(k + 1) * rows_out] = totals[k].astype(BF16)

    @pl.when(jnp.logical_not(own))
    def _():
        remote(obuf.at[s], rbuf.at[slot], c_send.at[0], c_recv.at[slot], (owner, s)).wait_send()

    for copy in sent[len(sent) - (n_s - 1):]:
        copy.wait_send()


def shards(n_e, n_s, tokens, expert_ids, gates, gate_proj, up_proj, down_proj_t):
    tok, width = tokens.shape
    _, _, hid = gate_proj.shape
    _, rows_out, _ = down_proj_t.shape
    chunks = max(1, hid // 256)
    wide = hid // chunks
    total = tok * n_s
    group = n_s // n_e
    dma = pltpu.SemaphoreType.DMA
    vmem = pl.BlockSpec(memory_space=pltpu.VMEM)
    hbm = pl.BlockSpec(memory_space=pl.ANY)
    return pl.pallas_call(
        functools.partial(kernel, n_e, n_s, chunks),
        out_shape=jax.ShapeDtypeStruct((tok, width), BF16),
        in_specs=[vmem, vmem, vmem, hbm, hbm, hbm],
        out_specs=vmem,
        scratch_shapes=[
            pltpu.VMEM((n_e, width, hid), BF16),
            pltpu.VMEM((n_e, width, hid), BF16),
            pltpu.VMEM((n_s, rows_out, hid), BF16),
            pltpu.VMEM((n_e, n_s, PAD, width), BF16),
            pltpu.VMEM((total, hid), F32),
            pltpu.VMEM((total, hid), F32),
            pltpu.VMEM((n_s, chunks, total, wide), BF16),
            pltpu.VMEM((total, rows_out), F32),
            pltpu.VMEM((n_s, PAD, rows_out), BF16),
            pltpu.VMEM((n_e * group, PAD, rows_out), BF16),
            dma((2, n_e)),
            dma((n_s,)),
            dma((n_e, n_s)),
            dma((n_e, n_s)),
            dma((2, n_s, chunks)),
            dma((n_s, chunks)),
            dma((n_s, chunks)),
            dma((n_s,)),
            dma((n_e * group,)),
        ],
        compiler_params=pltpu.CompilerParams(
            collective_id=0, has_side_effects=True, vmem_limit_bytes=60 * 1024 * 1024
        ),
    )(tokens, expert_ids.T, gates.T, gate_proj, up_proj, down_proj_t)


def solution(mesh):
    in_specs = (
        P("shard", "expert"),
        P("shard", None),
        P("shard", None),
        P("expert", None, "shard"),
        P("expert", None, "shard"),
        P("expert", "shard", None),
    )
    out_specs = P("shard", "expert")
    body = functools.partial(shards, mesh.shape["expert"], mesh.shape["shard"])
    return jax.shard_map(body, mesh=mesh, in_specs=in_specs, out_specs=out_specs, check_vma=False)
```

```python
import functools

import jax
import jax.numpy as jnp
from jax import lax
from jax.experimental import pallas as pl
from jax.experimental.pallas import tpu as pltpu
from jax.sharding import PartitionSpec as P

PAD = 8
MESH = pl.DeviceIdType.MESH
F32 = jnp.float32
BF16 = jnp.bfloat16


def flip(index, mask):
    bit, out = 1, index
    while bit <= mask:
        if mask & bit:
            out = out + bit - 2 * bit * ((index // bit) % 2)
        bit *= 2
    return out


def kernel(
    n_e, n_s, chunks,
    tok_ref, ids_ref, gates_ref, gate_hbm, up_hbm, down_hbm, out_ref,
    gbuf, ubuf, dbuf, x8, gacc, uacc, hbuf, oacc, obuf, rbuf,
    wsem, dsem, a_send, a_recv, h_send, h_fwd, h_recv, c_send, c_recv,
):
    e = lax.axis_index("expert")
    s = lax.axis_index("shard")
    tok, width = tok_ref.shape
    tokens = tok * n_s
    hid = gbuf.shape[2]
    wide = hid // chunks
    rows_out = dbuf.shape[1]
    group = n_s // n_e
    n_dev = n_e * n_s

    weight_copies, down_copies = [], []
    for r in range(n_e):
        rows = pl.ds(pl.multiple_of(flip(e, r) * width, width), width)
        pair = (
            pltpu.make_async_copy(gate_hbm.at[0, rows, :], gbuf.at[r], wsem.at[0, r]),
            pltpu.make_async_copy(up_hbm.at[0, rows, :], ubuf.at[r], wsem.at[1, r]),
        )
        for copy in pair:
            copy.start()
        weight_copies.append(pair)
    for q in range(n_s):
        columns = slice(q * hid, (q + 1) * hid)
        copy = pltpu.make_async_copy(down_hbm.at[0, :, columns], dbuf.at[q], dsem.at[q])
        copy.start()
        down_copies.append(copy)

    x8[0, s, :tok, :] = tok_ref[...]
    gacc[...] = jnp.zeros_like(gacc)
    uacc[...] = jnp.zeros_like(uacc)
    oacc[...] = jnp.zeros_like(oacc)

    barrier = pltpu.get_barrier_semaphore()
    me = e * n_s + s

    def greet(i, carry):
        other = lax.rem(me + i, n_dev)
        pl.semaphore_signal(
            barrier, inc=1, device_id=(other // n_s, other % n_s), device_id_type=MESH
        )
        return carry

    lax.fori_loop(1, n_dev, greet, 0)
    pl.semaphore_wait(barrier, n_dev - 1)

    sent = []

    def remote(src, dst, send, recv, device):
        return pltpu.make_async_remote_copy(
            src_ref=src, dst_ref=dst, send_sem=send, recv_sem=recv,
            device_id=device, device_id_type=MESH,
        )

    def push(*args):
        copy = remote(*args)
        copy.start()
        sent.append(copy)

    partner = (flip(e, 1), s)

    def filled(r, block):
        return x8.at[r, block, pl.ds(0, tok)]

    def onward(block):
        for r in range(2, n_e, 2):
            push(filled(0, block), filled(r, block), a_send.at[r, block], a_recv.at[r, block], (flip(e, r), s))
        push(filled(0, block), filled(1, block), a_send.at[1, block], a_recv.at[1, block], partner)

    def arrived(r, block):
        view = filled(r, block)
        remote(view, view, a_send.at[r, block], a_recv.at[r, block], partner).wait_recv()

    for q in sorted(range(1, n_s), reverse=True):
        push(filled(0, s), filled(0, s), a_send.at[0, flip(s, q)], a_recv.at[0, s], (e, flip(s, q)))
    onward(s)
    for q in range(1, n_s):
        block = flip(s, q)
        arrived(0, block)
        onward(block)

    padded = n_s * PAD
    i = lax.broadcasted_iota(jnp.int32, (tokens, padded), 0)
    j = lax.broadcasted_iota(jnp.int32, (tokens, padded), 1)
    block_of = lax.shift_right_logical(j, PAD.bit_length() - 1)
    pick = ((i == j - (PAD - tok) * block_of) & (j - PAD * block_of < tok)).astype(F32).astype(BF16)
    real = lax.rem(lax.broadcasted_iota(jnp.int32, (padded, width), 0), PAD) < tok
    line, side = s // 2, lax.rem(s, 2)
    across = (e, flip(s, 1))
    n_line = n_s // 2

    def send_along(place, c, step, k):
        beside = line + step

        @pl.when((beside >= 0) & (beside < n_line))
        def _():
            remote(hbuf.at[place, c], hbuf.at[place, c], h_send.at[k, place, c], h_recv.at[place, c],
                   (e, s + 2 * step)).start()

    def send_across(place, c):
        remote(hbuf.at[place, c], hbuf.at[place, c], h_fwd.at[place, c], h_recv.at[place, c], across).start()

    def project(r, last):
        whole = jnp.where(real, x8[r].astype(F32).reshape(padded, width), 0.0).astype(BF16)
        rows = jnp.dot(pick, whole, preferred_element_type=F32).astype(BF16)
        for copy in weight_copies[r]:
            copy.wait()
        for c in range(chunks):
            columns = slice(c * wide, (c + 1) * wide)
            g = gacc[:, columns] + jnp.dot(rows, gbuf[r, :, columns], preferred_element_type=F32)
            u = uacc[:, columns] + jnp.dot(rows, ubuf[r, :, columns], preferred_element_type=F32)
            if not last:
                gacc[:, columns] = g
                uacc[:, columns] = u
                continue
            hbuf[s, c] = (g / (1.0 + jnp.exp(-g)) * u).astype(BF16)
            send_across(s, c)
            send_along(s, c, 1, 0)
            send_along(s, c, -1, 1)

    project(0, n_e == 1)
    for q in range(n_s):
        arrived(1, flip(s, q))
    project(1, n_e == 2)
    for r in range(2, n_e, 2):
        for q in range(n_s):
            block = flip(s, q)
            arrived(r, block)
            push(filled(r, block), filled(r + 1, block), a_send.at[r + 1, block], a_recv.at[r + 1, block], partner)
        project(r, False)
    for r in range(3, n_e, 2):
        for q in range(n_s):
            arrived(r, flip(s, q))
        project(r, r == n_e - 1)

    for copy in down_copies:
        copy.wait()

    def down(place, c):
        columns = pl.ds(pl.multiple_of(c * wide, wide), wide)
        oacc[...] += lax.dot_general(
            hbuf[place, c], dbuf[place, :, columns], (((1,), (1,)), ((), ())),
            preferred_element_type=F32,
        )

    def landed(place, c):
        view = hbuf.at[place, c]
        remote(view, view, h_fwd.at[place, c], h_recv.at[place, c], across).wait_recv()

    inner = jnp.minimum(line, n_line - 1 - line)
    roomy = 1 - 2 * (line // ((n_line + 1) // 2))

    def event(t):
        paired = t < 2 * inner * chunks
        late = t - 2 * inner * chunks
        pair = t // 2
        away = jnp.where(paired, pair // chunks + 1, inner + 1 + late // chunks)
        c = jnp.where(paired, lax.rem(pair, chunks), lax.rem(late, chunks))
        sign = jnp.where(paired, 1 - 2 * lax.rem(t, 2), roomy)
        return line + sign * away, c, sign

    steps = (n_line - 1) * chunks

    def across_piece(t):
        spot, c, _ = event(t)
        return 2 * spot + 1 - side, c

    def along_piece(t):
        spot, c, _ = event(t)
        return 2 * spot + side, c

    def together(pieces, wait):
        total = oacc[...]
        for place, c in pieces:
            if wait:
                landed(place, c)
            columns = pl.ds(pl.multiple_of(c * wide, wide), wide)
            total += lax.dot_general(
                hbuf[place, c], dbuf[place, :, columns], (((1,), (1,)), ((), ())),
                preferred_element_type=F32,
            )
        oacc[...] = total

    def relay(t):
        spot, c, sign = event(t)
        place = 2 * spot + side
        landed(place, c)
        send_along(place, c, -sign, 0)
        send_across(place, c)

    first = min(chunks, steps)

    @pl.loop(0, first)
    def _(t):
        relay(t)
        down(s, t)

    for c in range(first, chunks):
        down(s, c)

    second = min(2 * chunks, steps)

    @pl.loop(first, second)
    def _(t):
        relay(t)
        landed(flip(s, 1), t - first)
        down(flip(s, 1), t - first)

    for c in range(second - first, chunks):
        landed(flip(s, 1), c)
        down(flip(s, 1), c)

    @pl.loop(second, steps)
    def _(t):
        relay(t)
        down(*along_piece(t - second))

    done = (steps - second) // chunks

    @pl.loop(done, n_line - 1)
    def _(k):
        together([along_piece(k * chunks + c) for c in range(chunks)], False)

    @pl.loop(0, n_line - 1)
    def _(k):
        together([across_piece(k * chunks + c) for c in range(chunks)], True)

    spread = pick.astype(F32).T.astype(BF16)
    blocks = jnp.dot(spread, oacc[...].astype(BF16), preferred_element_type=F32)
    obuf[...] = blocks.reshape(n_s, PAD, rows_out).astype(BF16)
    owner = s // group
    slot = e * group + lax.rem(s, group)
    own = e == owner

    @pl.when(own)
    def _():
        keep = pltpu.make_async_copy(obuf.at[s], rbuf.at[slot], c_recv.at[slot])
        keep.start()

    @pl.when(jnp.logical_not(own))
    def _():
        remote(obuf.at[s], rbuf.at[slot], c_send.at[0], c_recv.at[slot], (owner, s)).start()

    for q in range(1, n_s):
        other = flip(s, q)
        push(obuf.at[other], rbuf.at[slot], c_send.at[q], c_recv.at[slot], (owner, other))

    ids = ids_ref[...]
    gates = gates_ref[...]
    diagonal = lax.broadcasted_iota(jnp.int32, (tok, tok), 0) == lax.broadcasted_iota(jnp.int32, (tok, tok), 1)
    for copy in sent[:len(sent) - (n_s - 1)]:
        copy.wait_send()

    @pl.loop(0, chunks)
    def _(c):
        for k, step in ((0, 1), (1, -1)):
            beside_me = line + step

            @pl.when((beside_me >= 0) & (beside_me < n_line))
            def _():
                remote(hbuf.at[s, c], hbuf.at[s, c], h_send.at[k, s, c], h_recv.at[s, c], across).wait_send()

        remote(hbuf.at[s, c], hbuf.at[s, c], h_fwd.at[s, c], h_recv.at[s, c], across).wait_send()

    @pl.loop(0, steps)
    def _(t):
        spot, c, sign = event(t)
        place = 2 * spot + side
        view = hbuf.at[place, c]
        beside_me = line - sign

        @pl.when((beside_me >= 0) & (beside_me < n_line))
        def _():
            remote(view, view, h_send.at[0, place, c], h_recv.at[place, c], across).wait_send()

        remote(view, view, h_fwd.at[place, c], h_recv.at[place, c], across).wait_send()

    totals = [jnp.zeros((tok, rows_out), F32) for _ in range(group)]
    for x in range(n_e):
        row = jnp.sum(jnp.where(ids == x, gates, 0.0), axis=0, keepdims=True)
        weight = jnp.sum(jnp.where(diagonal, row, 0.0), axis=1, keepdims=True)
        for k in range(group):
            n = x * group + k
            remote(rbuf.at[n], rbuf.at[n], c_send.at[0], c_recv.at[n], partner).wait_recv()
            totals[k] = totals[k] + weight * rbuf[n].astype(F32)[:tok]
    for k in range(group):
        out_ref[:, k * rows_out:(k + 1) * rows_out] = totals[k].astype(BF16)

    @pl.when(jnp.logical_not(own))
    def _():
        remote(obuf.at[s], rbuf.at[slot], c_send.at[0], c_recv.at[slot], (owner, s)).wait_send()

    for copy in sent[len(sent) - (n_s - 1):]:
        copy.wait_send()


def shards(n_e, n_s, tokens, expert_ids, gates, gate_proj, up_proj, down_proj_t):
    tok, width = tokens.shape
    _, _, hid = gate_proj.shape
    _, rows_out, _ = down_proj_t.shape
    chunks = max(1, hid // 256)
    wide = hid // chunks
    total = tok * n_s
    group = n_s // n_e
    dma = pltpu.SemaphoreType.DMA
    vmem = pl.BlockSpec(memory_space=pltpu.VMEM)
    hbm = pl.BlockSpec(memory_space=pl.ANY)
    return pl.pallas_call(
        functools.partial(kernel, n_e, n_s, chunks),
        out_shape=jax.ShapeDtypeStruct((tok, width), BF16),
        in_specs=[vmem, vmem, vmem, hbm, hbm, hbm],
        out_specs=vmem,
        scratch_shapes=[
            pltpu.VMEM((n_e, width, hid), BF16),
            pltpu.VMEM((n_e, width, hid), BF16),
            pltpu.VMEM((n_s, rows_out, hid), BF16),
            pltpu.VMEM((n_e, n_s, PAD, width), BF16),
            pltpu.VMEM((total, hid), F32),
            pltpu.VMEM((total, hid), F32),
            pltpu.VMEM((n_s, chunks, total, wide), BF16),
            pltpu.VMEM((total, rows_out), F32),
            pltpu.VMEM((n_s, PAD, rows_out), BF16),
            pltpu.VMEM((n_e * group, PAD, rows_out), BF16),
            dma((2, n_e)),
            dma((n_s,)),
            dma((n_e, n_s)),
            dma((n_e, n_s)),
            dma((2, n_s, chunks)),
            dma((n_s, chunks)),
            dma((n_s, chunks)),
            dma((n_s,)),
            dma((n_e * group,)),
        ],
        compiler_params=pltpu.CompilerParams(
            collective_id=0, has_side_effects=True, vmem_limit_bytes=60 * 1024 * 1024
        ),
    )(tokens, expert_ids.T, gates.T, gate_proj, up_proj, down_proj_t)


def solution(mesh):
    in_specs = (
        P("shard", "expert"),
        P("shard", None),
        P("shard", None),
        P("expert", None, "shard"),
        P("expert", None, "shard"),
        P("expert", "shard", None),
    )
    out_specs = P("shard", "expert")
    body = functools.partial(shards, mesh.shape["expert"], mesh.shape["shard"])
    return jax.shard_map(body, mesh=mesh, in_specs=in_specs, out_specs=out_specs, check_vma=False)
```
